256 devices in a mesh: row: 16 (over y, z_hi), col: 16 (over x, z_lo, core).
Axes of the slice: x: 4, y: 4, z: 8 (z_hi: 4, z_lo: 2; z = z_hi * 2 + z_lo), core: 2. Of those that a mesh axis runs over, the one named last changes fastest.
Arguments:
- contact_map: float32 [2048, 2048], P('row', 'col'), may hold values from -6 to 6
- embed_weight: bfloat16 [16, 128], replicated, may hold values from -1.5 to 1.5
- embed_bias: float32 [128], replicated, may hold values from -3 to 3
- conv_weight: bfloat16 [3, 3, 3, 128, 128], replicated, may hold values from -0.1875 to 0.1875
- conv_bias: float32 [3, 128], replicated, may hold values from -3 to 3
- mix_weight: bfloat16 [128, 128], replicated, may hold values from -0.5 to 0.5
- mix_bias: float32 [128], replicated, may hold values from -6 to 6
- proj_weight: bfloat16 [128, 256], replicated, may hold values from -1 to 1
- proj_bias: float32 [256], replicated, may hold values from -3 to 3
- up_weight: bfloat16 [256, 1024], replicated, may hold values from -0.375 to 0.375
- up_bias: float32 [1024], replicated, may hold values from -3 to 3
- down_weight: bfloat16 [1024, 256], replicated, may hold values from -0.1875 to 0.1875
- down_bias: float32 [256], replicated, may hold values from -3 to 3
Outputs:
- latents: bfloat16 [512, 256], P(('row', 'col'))
- sym: bfloat16 [512, 512, 128], P('row', 'col')
The draws below stay inside these ranges and needn't reach their ends.
All inputs are finite; a program needn't handle non-finite values.
Results may differ from the reference program's by a relative error of at most 0.0085.
Values may be sent and summed in bfloat16 or wider, within the bound.
A program may use at most 64 MiB of HBM per device.

```python
import jax
import jax.numpy as jnp
from jax import lax

PATCH = 4
C = 128
L = 256
HID = 1024
LAYERS = 3
NP = 512
PIX = 2048


def shard_levels(stream_key, dims, cuts, smallest, top_value):
    gain, own = 1.0, jax.random.fold_in(stream_key, 6)
    for axis_at, shards_of in cuts:
        steps = jnp.exp(jax.random.uniform(jax.random.fold_in(own, axis_at), (shards_of,), jnp.float32, smallest / len(cuts), top_value / len(cuts)))
        gain = gain * jnp.repeat(steps, dims[axis_at] // shards_of).reshape([-1 if axis == axis_at else 1 for axis in range(len(dims))])
    return gain


def centred(rng, shape, spread, bound, shards=(), kind=jnp.bfloat16):
    values = jax.random.normal(rng, shape, jnp.float32) * spread
    if len(shards) > 0:
        values = shard_levels(rng, shape, shards, -0.22, 0.18) * values
    return jnp.clip(values, min=-bound, max=bound).astype(kind)


def setup_inputs(seed: int = 0) -> dict:
    keys = jax.random.split(jax.random.key(seed), 14)
    return {
        "contact_map": centred(keys[0], (PIX, PIX), 1.0, 6.0, ((0, 16), (1, 16)), jnp.float32),
        "embed_weight": centred(keys[1], (PATCH * PATCH, C), (PATCH * PATCH) ** -0.5, 1.5),
        "embed_bias": centred(keys[2], (C,), 0.5, 3.0, (), jnp.float32),
        "conv_weight": centred(keys[3], (LAYERS, 3, 3, C, C), (9 * C) ** -0.5, 0.1875),
        "conv_bias": centred(keys[4], (LAYERS, C), 0.5, 3.0, (), jnp.float32),
        "mix_weight": centred(keys[5], (C, C), C ** -0.5, 0.5),
        "mix_bias": centred(keys[6], (C,), 1.0, 6.0, (), jnp.float32),
        "proj_weight": centred(keys[7], (C, L), (C // 4) ** -0.5, 1.0),
        "proj_bias": centred(keys[8], (L,), 0.5, 3.0, (), jnp.float32),
        "up_weight": centred(keys[9], (L, HID), L ** -0.5, 0.375),
        "up_bias": centred(keys[10], (HID,), 0.5, 3.0, (), jnp.float32),
        "down_weight": centred(keys[11], (HID, L), HID ** -0.5, 0.1875),
        "down_bias": centred(keys[12], (L,), 0.5, 3.0, (), jnp.float32),
    }


def reference(contact_map, embed_weight, embed_bias, conv_weight, conv_bias, mix_weight, mix_bias, proj_weight, proj_bias, up_weight, up_bias, down_weight, down_bias):
    grid = contact_map.reshape(NP, PATCH, NP, PATCH).transpose(0, 2, 1, 3)
    patches = grid.reshape(NP * NP, PATCH * PATCH).astype(jnp.bfloat16)
    feat = jnp.dot(patches, embed_weight, preferred_element_type=jnp.float32) + embed_bias
    feat = feat.astype(jnp.bfloat16).reshape(NP, NP, C)
    for layer in range(LAYERS):
        lhs = feat.astype(jnp.float32)[None]
        rhs = conv_weight[layer].astype(jnp.float32)
        out = lax.conv_general_dilated(lhs, rhs, (1, 1), "SAME", dimension_numbers=("NHWC", "HWIO", "NHWC"), precision=lax.Precision.HIGHEST)[0]
        feat = jax.nn.gelu(out + conv_bias[layer]).astype(jnp.bfloat16)
    whole = feat.astype(jnp.float32)
    sym = ((whole + whole.transpose(1, 0, 2)) * 0.5).astype(jnp.bfloat16)
    mixed = jax.nn.gelu(jnp.dot(sym.reshape(NP * NP, C), mix_weight, preferred_element_type=jnp.float32) + mix_bias)
    pooled = (jnp.sum(mixed.reshape(NP, NP, C), axis=1) / NP).astype(jnp.bfloat16)
    latent = jnp.dot(pooled, proj_weight, preferred_element_type=jnp.float32) + proj_bias
    hidden = jax.nn.gelu(jnp.dot(latent.astype(jnp.bfloat16), up_weight, preferred_element_type=jnp.float32) + up_bias).astype(jnp.bfloat16)
    result = latent + jnp.dot(hidden, down_weight, preferred_element_type=jnp.float32) + down_bias
    return result.astype(jnp.bfloat16), sym
```

```python
import functools

import jax
import jax.numpy as jnp
from jax import lax
from jax.experimental import pallas as pl
from jax.experimental.pallas import tpu as pltpu
from jax.sharding import PartitionSpec as P

PATCH = 4
LAYERS = 3
TILE = 32
BLK = 8
PAD = 16
SUB = 48
CH = 128
MESH = pl.DeviceIdType.MESH
F32 = jnp.float32
BF16 = jnp.bfloat16
OFFSETS = [(dl, ds) for dl in (-1, 0, 1) for ds in (-1, 0, 1)]


def gelu(x):
    half = 0.5 * x
    inner = x * (0.7978845608028654 + (0.7978845608028654 * 0.044715) * (x * x))
    return half + half * jnp.tanh(inner)


def lead_src(d):
    return {-1: pl.ds(3, 1), 0: pl.ds(0, 4), 1: pl.ds(0, 1)}[d]


def lead_dst(d):
    return {-1: pl.ds(0, 1), 0: pl.ds(1, 4), 1: pl.ds(5, 1)}[d]


def sub_src(d):
    return {-1: pl.ds(TILE - PAD, PAD), 0: pl.ds(0, TILE), 1: pl.ds(0, PAD)}[d]


def sub_dst(d):
    return {-1: pl.ds(0, PAD), 0: pl.ds(PAD, TILE), 1: pl.ds(PAD + TILE, PAD)}[d]


def kernel(
    n,
    x_ref,
    ew_ref,
    eb_ref,
    cw_hbm,
    cb_ref,
    mw_ref,
    mb_ref,
    pw_hbm,
    pb_ref,
    uw_hbm,
    ub_ref,
    dw_hbm,
    db_ref,
    lat_ref,
    sym_hbm,
    xt,
    own_p,
    own_q,
    near_h,
    far_h,
    f0,
    f1,
    f2,
    f3,
    symb,
    cw,
    pw,
    uw,
    dw,
    part,
    got,
    near_ss,
    near_rs,
    far_ss,
    far_rs,
    red_ss,
    red_rs,
    wsem,
    osem,
):
    r = lax.axis_index("row")
    c = lax.axis_index("col")
    rows_each = TILE // n

    weights = [
        pltpu.make_async_copy(src, dst, wsem.at[k])
        for k, (src, dst) in enumerate([(cw_hbm, cw), (pw_hbm, pw), (uw_hbm, uw), (dw_hbm, dw)])
    ]
    for w in weights:
        w.start()

    def inside(a, b):
        return (a >= 0) & (a < n) & (b >= 0) & (b < n)

    barrier = pltpu.get_barrier_semaphore()
    count = jnp.int32(n - 1)

    def greet(a, b):
        pl.semaphore_signal(barrier, inc=1, device_id=(a, b), device_id_type=MESH)

    for dl, ds in OFFSETS:
        far_ok = inside(c + ds, r + dl) & ((c + ds != r) | (r + dl != c))
        pl.when(far_ok)(functools.partial(greet, c + ds, r + dl))
        count += far_ok.astype(jnp.int32)
    for dl, ds in OFFSETS:
        if dl or ds:
            near_ok = inside(r + dl, c + ds)
            pl.when(near_ok)(functools.partial(greet, r + dl, c + ds))
            count += near_ok.astype(jnp.int32)
    for k in range(1, n):
        greet(r, lax.rem(c + k, n))

    xt[...] = x_ref[...].T
    y_p = jnp.concatenate([x_ref[pl.ds(s, TILE, stride=PATCH), :] for s in range(PATCH)], axis=1)
    y_q = jnp.concatenate([xt[pl.ds(s, TILE, stride=PATCH), :] for s in range(PATCH)], axis=1)
    y = jnp.concatenate([y_p, y_q], axis=0).astype(BF16)
    k = lax.broadcasted_iota(jnp.int32, (512, 512), 0)
    target = ((k >> 5) & 3) * 128 + ((k >> 2) & 7) * 16 + (k >> 7) * 4 + (k & 3)
    perm = (lax.broadcasted_iota(jnp.int32, (512, 512), 1) == target).astype(F32).astype(BF16)
    z = jnp.dot(y, perm, preferred_element_type=F32).astype(BF16)
    for h in range(4):
        p_h = z[:TILE, h * 128 : (h + 1) * 128]
        q_h = z[TILE:, h * 128 : (h + 1) * 128]
        own_p[h] = p_h
        own_q[h] = q_h
        near_h[h + 1, PAD : PAD + TILE, :] = q_h

    pr = lax.broadcasted_iota(jnp.int32, (128, 16), 0)
    pc = lax.broadcasted_iota(jnp.int32, (128, 16), 1)
    rid = lax.broadcasted_iota(jnp.int32, (128, 128), 0) >> 4

    def block_diagonal(swap):
        row = (pr & 3) * 4 + ((pr >> 2) & 3) if swap else pr & 15
        pick = (pc == row).astype(F32).astype(BF16)
        tiled = jnp.dot(pick, ew_ref[...], preferred_element_type=F32)
        return jnp.concatenate(
            [jnp.where(rid == b, tiled, 0.0).astype(BF16) for b in range(BLK)], axis=1
        )

    pl.semaphore_wait(barrier, count)

    def message(src, dst, ss, rs, dl, ds, a, b):
        i = (dl + 1) * 3 + ds + 1
        return pltpu.make_async_remote_copy(
            src_ref=src.at[lead_src(dl), sub_src(ds), :],
            dst_ref=dst.at[lead_dst(dl), sub_dst(ds), :],
            send_sem=ss.at[i],
            recv_sem=rs.at[i],
            device_id=(a, b),
            device_id_type=MESH,
        )

    far_out, far_in, near_out, near_in = [], [], [], []
    for dl, ds in OFFSETS:
        a, b = c - dl, r - ds
        ok = inside(a, b) & ((a != r) | (b != c))
        out = message(own_p, far_h, far_ss, far_rs, dl, ds, a, b)
        far_out.append((ok, out))
        pl.when(ok)(out.start)
        ok_in = inside(c + ds, r + dl) & ((c + ds != r) | (r + dl != c))
        far_in.append((ok_in, message(own_p, far_h, far_ss, far_rs, dl, ds, r, c)))
    for dl, ds in OFFSETS:
        if dl or ds:
            a, b = r - dl, c - ds
            ok = inside(a, b)
            out = message(own_q, near_h, near_ss, near_rs, dl, ds, a, b)
            near_out.append((ok, out))
            pl.when(ok)(out.start)
            near_in.append(
                (inside(r + dl, c + ds), message(own_q, near_h, near_ss, near_rs, dl, ds, r, c))
            )

    def keep(dl, ds):
        far_h[lead_dst(dl), sub_dst(ds), :] = own_p[lead_src(dl), sub_src(ds), :]

    pl.when(r == c)(functools.partial(keep, 0, 0))
    pl.when(c == r + 1)(functools.partial(keep, 1, -1))
    pl.when(c == r - 1)(functools.partial(keep, -1, 1))

    sub_cell = c * TILE - 8 + lax.broadcasted_iota(jnp.int32, (1, SUB, 1), 1)
    sub_ok = (sub_cell >= 0) & (sub_cell < n * TILE)

    def masked(value, first):
        count_l = value.shape[0]
        lead = r * TILE + first + lax.broadcasted_iota(jnp.int32, (count_l, SUB, 1), 0)
        ok = sub_ok & (lead >= 0) & (lead < n * TILE)
        return jnp.where(ok, value, 0.0)

    def put(ref, at, value, cut=False):
        count_l = value.shape[0]
        flat = value.reshape(count_l * SUB, CH)
        for s in range(3):
            moved = flat if s == 1 else pltpu.roll(flat, 1 if s == 0 else count_l * SUB - 1, 0)
            moved = moved.reshape(count_l, SUB, CH)
            if cut:
                moved = moved[:, 8:40, :]
            ref[s, at : at + count_l] = moved.astype(BF16)

    def embed(patches, diag):
        for h in range(6):
            first, last = (5, 8) if h == 0 else (0, 3) if h == 5 else (0, 8)
            wide = jnp.dot(patches[h], diag, preferred_element_type=F32)
            cells = jnp.concatenate(
                [
                    (wide[8:56, b * CH : (b + 1) * CH] + eb_ref[...])[None]
                    for b in range(first, last)
                ],
                axis=0,
            )
            at = h * BLK + first - 5
            put(f0, at, masked(cells, at - 3))

    def conv(layer, src, at, count_l, lead_is_row):
        pieces = []
        for a in range(3):
            for b in range(3):
                lead, sub = (a, b) if lead_is_row else (b, a)
                piece = src[sub, at + lead : at + lead + count_l]
                pieces.append(piece.reshape(count_l * piece.shape[1], CH))
        lhs = jnp.concatenate(pieces, axis=1)
        total = jnp.dot(lhs, cw[layer], preferred_element_type=F32)
        return gelu(total + cb_ref[layer])

    def features(lead_is_row, finish):
        for at in range(0, 36, 12):
            v = conv(0, f0, at, 12, lead_is_row).reshape(12, SUB, CH)
            put(f1, at, masked(v, at - 2))
        for at in range(0, 34, 17):
            v = conv(1, f1, at, 17, lead_is_row).reshape(17, SUB, CH)
            put(f2, at, masked(v, at - 1), cut=True)
        for at in range(0, TILE, 16):
            finish(at, conv(2, f2, at, 16, lead_is_row).astype(BF16))

    diag_q = block_diagonal(True)
    for ok, got_in in near_in:
        pl.when(ok)(got_in.wait_recv)
    embed(near_h, diag_q)
    weights[0].wait()

    def keep_own(at, value):
        f3[at * TILE : (at + 16) * TILE, :] = value

    features(True, keep_own)

    diag_p = block_diagonal(False)
    for ok, got_in in far_in:
        pl.when(ok)(got_in.wait_recv)
    embed(far_h, diag_p)

    outs = []

    def finish_far(at, value):
        mean = (f3[at * TILE : (at + 16) * TILE, :].astype(F32) + value.astype(F32)) * 0.5
        sym = mean.astype(BF16)
        symb[at : at + 16] = sym.reshape(16, TILE, CH)
        out = pltpu.make_async_copy(symb.at[pl.ds(at, 16)], sym_hbm.at[pl.ds(at, 16)], osem.at[at // 16])
        out.start()
        outs.append(out)
        mixed = gelu(jnp.dot(sym, mw_ref[...], preferred_element_type=F32) + mb_ref[...])
        sums = jnp.sum(mixed.reshape(16, TILE, CH), axis=1)
        for g in range(16 // rows_each):
            part[at // rows_each + g] = sums[g * rows_each : (g + 1) * rows_each]

    features(False, finish_far)

    moves = []
    for k in range(1, n):
        to = lax.rem(c + k, n)
        move = pltpu.make_async_remote_copy(
            src_ref=part.at[to],
            dst_ref=got.at[k],
            send_sem=red_ss.at[k],
            recv_sem=red_rs.at[k],
            device_id=(r, to),
            device_id_type=MESH,
        )
        move.start()
        moves.append(move)
    for w in weights[1:]:
        w.wait()
    for move in moves:
        move.wait_recv()
    summed = part[c]
    for k in range(1, n):
        summed = summed + got[k]
    pooled = (summed / (n * TILE)).astype(BF16)
    latent = jnp.dot(pooled, pw[...], preferred_element_type=F32) + pb_ref[...]
    hidden = gelu(jnp.dot(latent.astype(BF16), uw[...], preferred_element_type=F32) + ub_ref[...])
    result = latent + jnp.dot(hidden.astype(BF16), dw[...], preferred_element_type=F32) + db_ref[...]
    lat_ref[...] = result.astype(BF16)

    for move in moves:
        move.wait_send()
    for ok, out in far_out + near_out:
        pl.when(ok)(out.wait_send)
    for out in outs:
        out.wait()


def body(
    contact_map,
    embed_weight,
    embed_bias,
    conv_weight,
    conv_bias,
    mix_weight,
    mix_bias,
    proj_weight,
    proj_bias,
    up_weight,
    up_bias,
    down_weight,
    down_bias,
):
    n = lax.axis_size("col")
    rows_each = TILE // n
    latent_width, hidden_width = up_weight.shape
    vmem = pl.BlockSpec(memory_space=pltpu.VMEM)
    hbm = pl.BlockSpec(memory_space=pl.ANY)
    dma = pltpu.SemaphoreType.DMA
    return pl.pallas_call(
        functools.partial(kernel, n),
        out_shape=(
            jax.ShapeDtypeStruct((rows_each, latent_width), BF16),
            jax.ShapeDtypeStruct((TILE, TILE, CH), BF16),
        ),
        in_specs=[vmem, vmem, vmem, hbm, vmem, vmem, vmem, hbm, vmem, hbm, vmem, hbm, vmem],
        out_specs=(vmem, hbm),
        scratch_shapes=[
            pltpu.VMEM((TILE * PATCH, TILE * PATCH), F32),
            pltpu.VMEM((4, TILE, 128), BF16),
            pltpu.VMEM((4, TILE, 128), BF16),
            pltpu.VMEM((6, TILE + 2 * PAD, 128), BF16),
            pltpu.VMEM((6, TILE + 2 * PAD, 128), BF16),
            pltpu.VMEM((3, 38, SUB, CH), BF16),
            pltpu.VMEM((3, 36, SUB, CH), BF16),
            pltpu.VMEM((3, 34, TILE, CH), BF16),
            pltpu.VMEM((TILE * TILE, CH), BF16),
            pltpu.VMEM((TILE, TILE, CH), BF16),
            pltpu.VMEM((LAYERS, 9 * CH, CH), BF16),
            pltpu.VMEM(proj_weight.shape, BF16),
            pltpu.VMEM(up_weight.shape, BF16),
            pltpu.VMEM(down_weight.shape, BF16),
            pltpu.VMEM((n, rows_each, CH), F32),
            pltpu.VMEM((n, rows_each, CH), F32),
            dma((9,)),
            dma((9,)),
            dma((9,)),
            dma((9,)),
            dma((n,)),
            dma((n,)),
            dma((4,)),
            dma((2,)),
        ],
        compiler_params=pltpu.CompilerParams(
            collective_id=0, has_side_effects=True, vmem_limit_bytes=48 * 1024 * 1024
        ),
    )(
        contact_map,
        embed_weight,
        embed_bias.reshape(1, CH),
        conv_weight.reshape(LAYERS, 9 * CH, CH),
        conv_bias.reshape(LAYERS, 1, CH),
        mix_weight,
        mix_bias.reshape(1, CH),
        proj_weight,
        proj_bias.reshape(1, latent_width),
        up_weight,
        up_bias.reshape(1, hidden_width),
        down_weight,
        down_bias.reshape(1, latent_width),
    )


def solution(mesh):
    return jax.shard_map(
        body,
        mesh=mesh,
        in_specs=(P("row", "col"),) + (P(),) * 12,
        out_specs=(P(("row", "col"), None), P("row", "col", None)),
        check_vma=False,
    )
```

```python
import functools

import jax
import jax.numpy as jnp
from jax import lax
from jax.experimental import pallas as pl
from jax.experimental.pallas import tpu as pltpu
from jax.sharding import PartitionSpec as P

PATCH = 4
LAYERS = 3
TILE = 32
BLK = 8
PAD = 8
SUB = 48
CH = 128
MESH = pl.DeviceIdType.MESH
F32 = jnp.float32
BF16 = jnp.bfloat16
OFFSETS = [(dl, ds) for dl in (-1, 0, 1) for ds in (-1, 0, 1)]


def gelu(x):
    half = 0.5 * x
    inner = x * (0.7978845608028654 + (0.7978845608028654 * 0.044715) * (x * x))
    return half + half * jnp.tanh(inner)


def lead_src(d):
    return {-1: pl.ds(3, 1), 0: pl.ds(0, 4), 1: pl.ds(0, 1)}[d]


def lead_dst(d):
    return {-1: pl.ds(0, 1), 0: pl.ds(1, 4), 1: pl.ds(5, 1)}[d]


def sub_src(d):
    return {-1: pl.ds(TILE - PAD, PAD), 0: pl.ds(0, TILE), 1: pl.ds(0, PAD)}[d]


def sub_dst(d):
    return {-1: pl.ds(0, PAD), 0: pl.ds(PAD, TILE), 1: pl.ds(PAD + TILE, PAD)}[d]


def kernel(
    n,
    x_hbm,
    ew_hbm,
    eb_hbm,
    cw_hbm,
    cb_hbm,
    mw_hbm,
    mb_hbm,
    pw_hbm,
    pb_hbm,
    uw_hbm,
    ub_hbm,
    dw_hbm,
    db_hbm,
    lat_hbm,
    sym_hbm,
    x_ref,
    ew_ref,
    eb_ref,
    cw,
    cb_ref,
    mw_ref,
    mb_ref,
    pw,
    pb_ref,
    uw,
    ub_ref,
    dw,
    db_ref,
    xt,
    own_p,
    own_q,
    near_h,
    far_h,
    f0,
    f1,
    f2,
    f3,
    symb,
    lat_ref,
    part,
    got,
    near_ss,
    near_rs,
    far_ss,
    far_rs,
    red_ss,
    red_rs,
    wsem,
    osem,
):
    r = lax.axis_index("row")
    c = lax.axis_index("col")
    rows_each = TILE // n

    held = [
        (x_hbm, x_ref),
        (ew_hbm, ew_ref),
        (eb_hbm, eb_ref),
        (cw_hbm, cw),
        (cb_hbm, cb_ref),
        (mw_hbm, mw_ref),
        (mb_hbm, mb_ref),
        (pw_hbm, pw),
        (pb_hbm, pb_ref),
        (uw_hbm, uw),
        (ub_hbm, ub_ref),
        (dw_hbm, dw),
        (db_hbm, db_ref),
    ]
    loads = [pltpu.make_async_copy(src, dst, wsem.at[k]) for k, (src, dst) in enumerate(held)]
    for load in loads:
        load.start()

    def inside(a, b):
        return (a >= 0) & (a < n) & (b >= 0) & (b < n)

    barrier = pltpu.get_barrier_semaphore()
    count = jnp.int32(n - 1)

    def greet(a, b):
        pl.semaphore_signal(barrier, inc=1, device_id=(a, b), device_id_type=MESH)

    for dl, ds in OFFSETS:
        far_ok = inside(c + ds, r + dl) & ((c + ds != r) | (r + dl != c))
        pl.when(far_ok)(functools.partial(greet, c + ds, r + dl))
        count += far_ok.astype(jnp.int32)
    for dl, ds in OFFSETS:
        if dl or ds:
            near_ok = inside(r + dl, c + ds)
            pl.when(near_ok)(functools.partial(greet, r + dl, c + ds))
            count += near_ok.astype(jnp.int32)
    for k in range(1, n):
        greet(r, lax.rem(c + k, n))

    loads[0].wait()
    xt[...] = x_ref[...].T
    y_p = jnp.concatenate([x_ref[pl.ds(s, TILE, stride=PATCH), :] for s in range(PATCH)], axis=1)
    y_q = jnp.concatenate([xt[pl.ds(s, TILE, stride=PATCH), :] for s in range(PATCH)], axis=1)
    y = jnp.concatenate([y_p, y_q], axis=0).astype(BF16)
    k = lax.broadcasted_iota(jnp.int32, (512, 512), 0)
    target = ((k >> 5) & 3) * 128 + ((k >> 2) & 7) * 16 + (k >> 7) * 4 + (k & 3)
    perm = (lax.broadcasted_iota(jnp.int32, (512, 512), 1) == target).astype(F32).astype(BF16)
    z = jnp.dot(y, perm, preferred_element_type=F32).astype(BF16)
    for h in range(4):
        p_h = z[:TILE, h * 128 : (h + 1) * 128]
        q_h = z[TILE:, h * 128 : (h + 1) * 128]
        own_p[h] = p_h
        own_q[h] = q_h
        near_h[h + 1, PAD : PAD + TILE, :] = q_h

    for load in loads[1:]:
        load.wait()
    pr = lax.broadcasted_iota(jnp.int32, (128, 16), 0)
    pc = lax.broadcasted_iota(jnp.int32, (128, 16), 1)
    rid = lax.broadcasted_iota(jnp.int32, (128, 128), 0) >> 4

    def block_diagonal(swap):
        row = (pr & 3) * 4 + ((pr >> 2) & 3) if swap else pr & 15
        pick = (pc == row).astype(F32).astype(BF16)
        tiled = jnp.dot(pick, ew_ref[...], preferred_element_type=F32)
        return jnp.concatenate(
            [jnp.where(rid == b, tiled, 0.0).astype(BF16) for b in range(BLK)], axis=1
        )

    pl.semaphore_wait(barrier, count)

    def message(src, dst, ss, rs, dl, ds, a, b):
        i = (dl + 1) * 3 + ds + 1
        return pltpu.make_async_remote_copy(
            src_ref=src.at[lead_src(dl), sub_src(ds), :],
            dst_ref=dst.at[lead_dst(dl), sub_dst(ds), :],
            send_sem=ss.at[i],
            recv_sem=rs.at[i],
            device_id=(a, b),
            device_id_type=MESH,
        )

    far_out, far_in, near_out, near_in = [], [], [], []
    for dl, ds in OFFSETS:
        a, b = c - dl, r - ds
        ok = inside(a, b) & ((a != r) | (b != c))
        out = message(own_p, far_h, far_ss, far_rs, dl, ds, a, b)
        far_out.append((ok, out))
        pl.when(ok)(out.start)
        ok_in = inside(c + ds, r + dl) & ((c + ds != r) | (r + dl != c))
        far_in.append((ok_in, message(own_p, far_h, far_ss, far_rs, dl, ds, r, c)))
    for dl, ds in OFFSETS:
        if dl or ds:
            a, b = r - dl, c - ds
            ok = inside(a, b)
            out = message(own_q, near_h, near_ss, near_rs, dl, ds, a, b)
            near_out.append((ok, out))
            pl.when(ok)(out.start)
            near_in.append(
                (inside(r + dl, c + ds), message(own_q, near_h, near_ss, near_rs, dl, ds, r, c))
            )

    def keep(dl, ds):
        far_h[lead_dst(dl), sub_dst(ds), :] = own_p[lead_src(dl), sub_src(ds), :]

    pl.when(r == c)(functools.partial(keep, 0, 0))
    pl.when(c == r + 1)(functools.partial(keep, 1, -1))
    pl.when(c == r - 1)(functools.partial(keep, -1, 1))

    sub_cell = c * TILE - 8 + lax.broadcasted_iota(jnp.int32, (1, SUB, 1), 1)
    sub_ok = (sub_cell >= 0) & (sub_cell < n * TILE)

    def masked(value, first):
        count_l = value.shape[0]
        lead = r * TILE + first + lax.broadcasted_iota(jnp.int32, (count_l, SUB, 1), 0)
        ok = sub_ok & (lead >= 0) & (lead < n * TILE)
        return jnp.where(ok, value, 0.0)

    def put(ref, at, value, cut=False):
        count_l = value.shape[0]
        flat = value.reshape(count_l * SUB, CH)
        for s in range(3):
            moved = flat if s == 1 else pltpu.roll(flat, 1 if s == 0 else count_l * SUB - 1, 0)
            moved = moved.reshape(count_l, SUB, CH)
            if cut:
                moved = moved[:, 8:40, :]
            ref[s, at : at + count_l] = moved.astype(BF16)

    def embed(patches, diag):
        for h in range(6):
            first, last = (5, 8) if h == 0 else (0, 3) if h == 5 else (0, 8)
            wide = jnp.dot(patches[h], diag, preferred_element_type=F32)
            cells = jnp.concatenate(
                [
                    (wide[:, b * CH : (b + 1) * CH] + eb_ref[...])[None]
                    for b in range(first, last)
                ],
                axis=0,
            )
            at = h * BLK + first - 5
            put(f0, at, masked(cells, at - 3))

    def conv(layer, src, at, count_l, lead_is_row):
        pieces = []
        for a in range(3):
            for b in range(3):
                lead, sub = (a, b) if lead_is_row else (b, a)
                piece = src[sub, at + lead : at + lead + count_l]
                pieces.append(piece.reshape(count_l * piece.shape[1], CH))
        lhs = jnp.concatenate(pieces, axis=1)
        total = jnp.dot(lhs, cw[layer], preferred_element_type=F32)
        return gelu(total + cb_ref[layer : layer + 1])

    def features(lead_is_row, finish):
        for at in range(0, 36, 12):
            v = conv(0, f0, at, 12, lead_is_row).reshape(12, SUB, CH)
            put(f1, at, masked(v, at - 2))
        for at in range(0, 34, 17):
            v = conv(1, f1, at, 17, lead_is_row).reshape(17, SUB, CH)
            put(f2, at, masked(v, at - 1), cut=True)
        for at in range(0, TILE, 16):
            finish(at, conv(2, f2, at, 16, lead_is_row).astype(BF16))

    diag_q = block_diagonal(True)
    for ok, got_in in near_in:
        pl.when(ok)(got_in.wait_recv)
    embed(near_h, diag_q)

    def keep_own(at, value):
        f3[at * TILE : (at + 16) * TILE, :] = value

    features(True, keep_own)

    diag_p = block_diagonal(False)
    for ok, got_in in far_in:
        pl.when(ok)(got_in.wait_recv)
    embed(far_h, diag_p)

    outs = []

    def finish_far(at, value):
        mean = (f3[at * TILE : (at + 16) * TILE, :].astype(F32) + value.astype(F32)) * 0.5
        sym = mean.astype(BF16)
        symb[at : at + 16] = sym.reshape(16, TILE, CH)
        out = pltpu.make_async_copy(
            symb.at[pl.ds(at, 16)], sym_hbm.at[pl.ds(at, 16)], osem.at[at // 16]
        )
        out.start()
        outs.append(out)
        mixed = gelu(jnp.dot(sym, mw_ref[...], preferred_element_type=F32) + mb_ref[...])
        sums = jnp.sum(mixed.reshape(16, TILE, CH), axis=1)
        for g in range(16 // rows_each):
            part[at // rows_each + g] = sums[g * rows_each : (g + 1) * rows_each]

    features(False, finish_far)

    moves = []
    for k in range(1, n):
        to = lax.rem(c + k, n)
        move = pltpu.make_async_remote_copy(
            src_ref=part.at[to],
            dst_ref=got.at[k],
            send_sem=red_ss.at[k],
            recv_sem=red_rs.at[k],
            device_id=(r, to),
            device_id_type=MESH,
        )
        move.start()
        moves.append(move)
    for move in moves:
        move.wait_recv()
    summed = part[c]
    for k in range(1, n):
        summed = summed + got[k]
    pooled = (summed / (n * TILE)).astype(BF16)
    latent = jnp.dot(pooled, pw[...], preferred_element_type=F32) + pb_ref[...]
    hidden = gelu(jnp.dot(latent.astype(BF16), uw[...], preferred_element_type=F32) + ub_ref[...])
    result = latent + jnp.dot(hidden.astype(BF16), dw[...], preferred_element_type=F32) + db_ref[...]
    lat_ref[...] = result.astype(BF16)
    out = pltpu.make_async_copy(lat_ref, lat_hbm, osem.at[2])
    out.start()
    outs.append(out)

    for move in moves:
        move.wait_send()
    for ok, out in far_out + near_out:
        pl.when(ok)(out.wait_send)
    for out in outs:
        out.wait()


def hand_over(lat_ref, sym_ref, lat_out, sym_out, lat_held, sym_held, sem_in, sem_out):
    steps = [(lat_ref, lat_held, lat_out)]
    for k in range(0, TILE, TILE // 4):
        part = pl.ds(k, TILE // 4)
        steps.append((sym_ref.at[part], sym_held.at[part], sym_out.at[part]))
    takes = [
        pltpu.make_async_copy(src, mid, sem_in.at[k]) for k, (src, mid, _) in enumerate(steps)
    ]
    gives = [
        pltpu.make_async_copy(mid, dst, sem_out.at[k]) for k, (_, mid, dst) in enumerate(steps)
    ]
    for take in takes:
        take.start()
    for take, give in zip(takes, gives):
        take.wait()
        give.start()
    for give in gives:
        give.wait()


def body(
    contact_map,
    embed_weight,
    embed_bias,
    conv_weight,
    conv_bias,
    mix_weight,
    mix_bias,
    proj_weight,
    proj_bias,
    up_weight,
    up_bias,
    down_weight,
    down_bias,
):
    n = lax.axis_size("col")
    rows_each = TILE // n
    latent_width, hidden_width = up_weight.shape
    vmem = pl.BlockSpec(memory_space=pltpu.VMEM)
    hbm = pl.BlockSpec(memory_space=pltpu.HBM)
    dma = pltpu.SemaphoreType.DMA
    args = (
        contact_map,
        embed_weight,
        embed_bias.reshape(1, CH),
        conv_weight.reshape(LAYERS, 9 * CH, CH),
        conv_bias,
        mix_weight,
        mix_bias.reshape(1, CH),
        proj_weight,
        proj_bias.reshape(1, latent_width),
        up_weight,
        up_bias.reshape(1, hidden_width),
        down_weight,
        down_bias.reshape(1, latent_width),
    )
    shapes = (
        jax.ShapeDtypeStruct((rows_each, latent_width), BF16),
        jax.ShapeDtypeStruct((TILE, TILE, CH), BF16),
    )
    done = pl.pallas_call(
        functools.partial(kernel, n),
        out_shape=shapes,
        in_specs=[hbm] * len(args),
        out_specs=(hbm, hbm),
        scratch_shapes=[pltpu.VMEM(a.shape, a.dtype) for a in args]
        + [
            pltpu.VMEM((TILE * PATCH, TILE * PATCH), F32),
            pltpu.VMEM((4, TILE, 128), BF16),
            pltpu.VMEM((4, TILE, 128), BF16),
            pltpu.VMEM((6, TILE + 2 * PAD, 128), BF16),
            pltpu.VMEM((6, TILE + 2 * PAD, 128), BF16),
            pltpu.VMEM((3, 38, SUB, CH), BF16),
            pltpu.VMEM((3, 36, SUB, CH), BF16),
            pltpu.VMEM((3, 34, TILE, CH), BF16),
            pltpu.VMEM((TILE * TILE, CH), BF16),
            pltpu.VMEM(shapes[1].shape, BF16),
            pltpu.VMEM(shapes[0].shape, BF16),
            pltpu.VMEM((n, rows_each, CH), F32),
            pltpu.VMEM((n, rows_each, CH), F32),
            dma((9,)),
            dma((9,)),
            dma((9,)),
            dma((9,)),
            dma((n,)),
            dma((n,)),
            dma((len(args),)),
            dma((3,)),
        ],
        compiler_params=pltpu.CompilerParams(
            collective_id=0, has_side_effects=True, vmem_limit_bytes=67043328
        ),
    )(*args)
    return pl.pallas_call(
        hand_over,
        out_shape=shapes,
        in_specs=[hbm, hbm],
        out_specs=(hbm, hbm),
        scratch_shapes=[pltpu.VMEM(shape.shape, BF16) for shape in shapes]
        + [dma((5,)), dma((5,))],
    )(*done)


def solution(mesh):
    return jax.shard_map(
        body,
        mesh=mesh,
        in_specs=(P("row", "col"),) + (P(),) * 12,
        out_specs=(P(("row", "col"), None), P("row", "col", None)),
        check_vma=False,
    )
```

```python
import functools

import jax
import jax.numpy as jnp
from jax import lax
from jax.experimental import pallas as pl
from jax.experimental.pallas import tpu as pltpu
from jax.sharding import PartitionSpec as P

PATCH = 4
LAYERS = 3
TILE = 32
BLK = 8
PAD = 8
SUB = 48
CH = 128
MESH = pl.DeviceIdType.MESH
F32 = jnp.float32
BF16 = jnp.bfloat16
CUTS = [[(0, 9), (9, 9)], [(0, 9), (9, 8)], [(0, 8), (8, 8)]]
OFFSETS = [(dl, ds) for dl in (-1, 0, 1) for ds in (-1, 0, 1)]


def gelu(x):
    half = 0.5 * x
    inner = x * (0.7978845608028654 + (0.7978845608028654 * 0.044715) * (x * x))
    return half + half * jnp.tanh(inner)


def lead_src(d):
    return {-1: pl.ds(3, 1), 0: pl.ds(0, 4), 1: pl.ds(0, 1)}[d]


def lead_dst(d):
    return {-1: pl.ds(0, 1), 0: pl.ds(1, 4), 1: pl.ds(5, 1)}[d]


def sub_src(d):
    return {-1: pl.ds(TILE - PAD, PAD), 0: pl.ds(0, TILE), 1: pl.ds(0, PAD)}[d]


def sub_dst(d):
    return {-1: pl.ds(0, PAD), 0: pl.ds(PAD, TILE), 1: pl.ds(PAD + TILE, PAD)}[d]


def kernel(
    n,
    x_hbm,
    ew_hbm,
    eb_hbm,
    cw_hbm,
    cb_hbm,
    mw_hbm,
    mb_hbm,
    pw_hbm,
    pb_hbm,
    uw_hbm,
    ub_hbm,
    dw_hbm,
    db_hbm,
    lat_hbm,
    sym_hbm,
    x_ref,
    ew_ref,
    eb_ref,
    cw,
    cb_ref,
    mw_ref,
    mb_ref,
    pw,
    pb_ref,
    uw,
    ub_ref,
    dw,
    db_ref,
    xt,
    own_p,
    own_q,
    near_h,
    far_h,
    f0,
    f1,
    f2,
    f3,
    acc,
    symb,
    lat_ref,
    part,
    got,
    near_ss,
    near_rs,
    far_ss,
    far_rs,
    red_ss,
    red_rs,
    wsem,
    osem,
):
    r = lax.axis_index("row")
    c = lax.axis_index("col")
    rows_each = TILE // n

    held = [
        (x_hbm, x_ref),
        (ew_hbm, ew_ref),
        (eb_hbm, eb_ref),
        (cw_hbm, cw),
        (cb_hbm, cb_ref),
        (mw_hbm, mw_ref),
        (mb_hbm, mb_ref),
        (pw_hbm, pw),
        (pb_hbm, pb_ref),
        (uw_hbm, uw),
        (ub_hbm, ub_ref),
        (dw_hbm, dw),
        (db_hbm, db_ref),
    ]
    def inside(a, b):
        return (a >= 0) & (a < n) & (b >= 0) & (b < n)

    barrier = pltpu.get_barrier_semaphore()
    count = jnp.int32(n - 1)

    def greet(a, b):
        pl.semaphore_signal(barrier, inc=1, device_id=(a, b), device_id_type=MESH)

    for dl, ds in OFFSETS:
        far_ok = inside(c + ds, r + dl) & ((c + ds != r) | (r + dl != c))
        pl.when(far_ok)(functools.partial(greet, c + ds, r + dl))
        count += far_ok.astype(jnp.int32)
    for dl, ds in OFFSETS:
        if dl or ds:
            near_ok = inside(r + dl, c + ds)
            pl.when(near_ok)(functools.partial(greet, r + dl, c + ds))
            count += near_ok.astype(jnp.int32)
    for k in range(1, n):
        greet(r, lax.rem(c + k, n))

    loads = [pltpu.make_async_copy(src, dst, wsem.at[k]) for k, (src, dst) in enumerate(held)]
    for load in loads:
        load.start()
    loads[0].wait()
    xt[...] = x_ref[...].T
    y_p = jnp.concatenate([x_ref[pl.ds(s, TILE, stride=PATCH), :] for s in range(PATCH)], axis=1)
    y_q = jnp.concatenate([xt[pl.ds(s, TILE, stride=PATCH), :] for s in range(PATCH)], axis=1)
    y = jnp.concatenate([y_p, y_q], axis=0).astype(BF16)
    k = lax.broadcasted_iota(jnp.int32, (512, 512), 0)
    target = ((k >> 5) & 3) * 128 + ((k >> 2) & 7) * 16 + (k >> 7) * 4 + (k & 3)
    perm = (lax.broadcasted_iota(jnp.int32, (512, 512), 1) == target).astype(F32).astype(BF16)
    z = jnp.dot(y, perm, preferred_element_type=F32).astype(BF16)
    for h in range(4):
        p_h = z[:TILE, h * 128 : (h + 1) * 128]
        q_h = z[TILE:, h * 128 : (h + 1) * 128]
        own_p[h] = p_h
        own_q[h] = q_h
        near_h[h + 1, PAD : PAD + TILE, :] = q_h

    for load in loads[1:]:
        load.wait()
    pr = lax.broadcasted_iota(jnp.int32, (128, 16), 0)
    pc = lax.broadcasted_iota(jnp.int32, (128, 16), 1)
    rid = lax.broadcasted_iota(jnp.int32, (128, 128), 0) >> 4

    def block_diagonal(swap):
        row = (pr & 3) * 4 + ((pr >> 2) & 3) if swap else pr & 15
        pick = (pc == row).astype(F32).astype(BF16)
        tiled = jnp.dot(pick, ew_ref[...], preferred_element_type=F32)
        return jnp.concatenate(
            [jnp.where(rid == b, tiled, 0.0).astype(BF16) for b in range(BLK)], axis=1
        )

    pl.semaphore_wait(barrier, count)

    def message(src, dst, ss, rs, dl, ds, a, b):
        i = (dl + 1) * 3 + ds + 1
        return pltpu.make_async_remote_copy(
            src_ref=src.at[lead_src(dl), sub_src(ds), :],
            dst_ref=dst.at[lead_dst(dl), sub_dst(ds), :],
            send_sem=ss.at[i],
            recv_sem=rs.at[i],
            device_id=(a, b),
            device_id_type=MESH,
        )

    far_out, far_in, near_out, near_in = [], [], [], []
    for dl, ds in OFFSETS:
        a, b = c - dl, r - ds
        ok = inside(a, b) & ((a != r) | (b != c))
        out = message(own_p, far_h, far_ss, far_rs, dl, ds, a, b)
        far_out.append((ok, out))
        pl.when(ok)(out.start)
        ok_in = inside(c + ds, r + dl) & ((c + ds != r) | (r + dl != c))
        far_in.append((ok_in, message(own_p, far_h, far_ss, far_rs, dl, ds, r, c)))
    for dl, ds in OFFSETS:
        if dl or ds:
            a, b = r - dl, c - ds
            ok = inside(a, b)
            out = message(own_q, near_h, near_ss, near_rs, dl, ds, a, b)
            near_out.append((ok, out))
            pl.when(ok)(out.start)
            near_in.append(
                (inside(r + dl, c + ds), message(own_q, near_h, near_ss, near_rs, dl, ds, r, c))
            )

    def keep(dl, ds):
        far_h[lead_dst(dl), sub_dst(ds), :] = own_p[lead_src(dl), sub_src(ds), :]

    pl.when(r == c)(functools.partial(keep, 0, 0))
    pl.when(c == r + 1)(functools.partial(keep, 1, -1))
    pl.when(c == r - 1)(functools.partial(keep, -1, 1))

    sub_cell = c * TILE - 8 + lax.broadcasted_iota(jnp.int32, (1, SUB, 1), 1)
    sub_ok = (sub_cell >= 0) & (sub_cell < n * TILE)

    def masked(value, first):
        count_l = value.shape[0]
        lead = r * TILE + first + 2 * lax.broadcasted_iota(jnp.int32, (count_l, SUB, 1), 0)
        ok = sub_ok & (lead >= 0) & (lead < n * TILE)
        return jnp.where(ok, value, 0.0)

    def put(ref, parity, at, value, cut=False):
        count_l = value.shape[0]
        flat = value.reshape(count_l * SUB, CH)
        for s in range(3):
            moved = flat if s == 1 else pltpu.roll(flat, 1 if s == 0 else count_l * SUB - 1, 0)
            moved = moved.reshape(count_l, SUB, CH)
            if cut:
                moved = moved[:, 8:40, :]
            ref[s, parity, at : at + count_l] = moved.astype(BF16)

    def embed(patches, diag):
        for h in range(6):
            first, last = (5, 8) if h == 0 else (0, 3) if h == 5 else (0, 8)
            wide = jnp.dot(patches[h], diag, preferred_element_type=F32)
            for start in (first, first + 1):
                cells = jnp.concatenate(
                    [
                        (wide[:, b * CH : (b + 1) * CH] + eb_ref[...])[None]
                        for b in range(start, last, 2)
                    ],
                    axis=0,
                )
                at = h * BLK + start - 5
                put(f0, at % 2, at // 2, masked(cells, at - 3))

    def conv(layer, src, at, pairs, lead_is_row, slot):
        def tap(lead, sub):
            if lead < 0 or lead > 2:
                return jnp.zeros((CH, CH), BF16)
            k = lead * 3 + sub if lead_is_row else sub * 3 + lead
            return cw[layer, k * CH : (k + 1) * CH, :]

        pieces, taps = [], []
        for lead in range(4):
            for sub in range(3):
                first = at + lead // 2
                piece = src[sub, lead % 2, first : first + pairs]
                pieces.append(piece.reshape(pairs * piece.shape[1], CH))
                taps.append(jnp.concatenate([tap(lead, sub), tap(lead - 1, sub)], axis=1))
        lhs = jnp.concatenate(pieces, axis=1)
        rows = pairs * SUB if layer < 2 else pairs * TILE
        acc[slot, :rows] = jnp.dot(lhs, jnp.concatenate(taps, axis=0), preferred_element_type=F32)

    def cell_row(layer, slot, k, h):
        each = SUB if layer < 2 else TILE
        total = acc[slot, k * each : (k + 1) * each, h * CH : (h + 1) * CH]
        return gelu(total + cb_ref[layer : layer + 1])

    def features(lead_is_row, finish):
        slot = 0
        for layer, (src, dst) in enumerate([(f0, f1), (f1, f2), (f2, None)]):
            for at, pairs in CUTS[layer]:
                conv(layer, src, at, pairs, lead_is_row, slot)
                for k in range(pairs):
                    for h in (0, 1):
                        v = cell_row(layer, slot, k, h)
                        if dst is None:
                            finish(at + k, h, v.astype(BF16))
                        else:
                            lead = 2 * (at + k) + h - 2 + layer
                            put(dst, h, at + k, masked(v[None], lead), cut=layer == 1)
                slot = 1 - slot

    diag_q = block_diagonal(True)
    for ok, got_in in near_in:
        pl.when(ok)(got_in.wait_recv)
    embed(near_h, diag_q)

    def keep_own(m, h, value):
        f3[2 * m + h] = value

    features(True, keep_own)

    diag_p = block_diagonal(False)
    for ok, got_in in far_in:
        pl.when(ok)(got_in.wait_recv)
    embed(far_h, diag_p)

    outs = []

    def finish_far(m, h, value):
        i = 2 * m + h
        symb[i] = ((f3[i].astype(F32) + value.astype(F32)) * 0.5).astype(BF16)

    features(False, finish_far)
    for at in range(0, TILE, 8):
        rows = pl.ds(at, 8)
        out = pltpu.make_async_copy(symb.at[rows], sym_hbm.at[rows], osem.at[at // 8])
        out.start()
        outs.append(out)
        mixed = jnp.dot(
            symb[rows].reshape(8 * TILE, CH), mw_ref[...], preferred_element_type=F32
        )
        sums = jnp.sum(gelu(mixed + mb_ref[...]).reshape(8, TILE, CH), axis=1)
        for k in range(8):
            row = at + k
            part[row // rows_each, row % rows_each : row % rows_each + 1] = sums[k : k + 1]

    moves = []
    for k in range(1, n):
        to = lax.rem(c + k, n)
        move = pltpu.make_async_remote_copy(
            src_ref=part.at[to],
            dst_ref=got.at[k],
            send_sem=red_ss.at[k],
            recv_sem=red_rs.at[k],
            device_id=(r, to),
            device_id_type=MESH,
        )
        move.start()
        moves.append(move)
    for move in moves:
        move.wait_recv()
    summed = part[c]
    for k in range(1, n):
        summed = summed + got[k]
    pooled = (summed / (n * TILE)).astype(BF16)
    latent = jnp.dot(pooled, pw[...], preferred_element_type=F32) + pb_ref[...]
    hidden = gelu(jnp.dot(latent.astype(BF16), uw[...], preferred_element_type=F32) + ub_ref[...])
    result = latent + jnp.dot(hidden.astype(BF16), dw[...], preferred_element_type=F32) + db_ref[...]
    lat_ref[...] = result.astype(BF16)
    out = pltpu.make_async_copy(lat_ref, lat_hbm, osem.at[len(outs)])
    out.start()
    outs.append(out)

    for move in moves:
        move.wait_send()
    for ok, out in far_out + near_out:
        pl.when(ok)(out.wait_send)
    for out in outs:
        out.wait()


def hand_over(lat_ref, sym_ref, lat_out, sym_out, lat_held, sym_held, sem_in, sem_out):
    steps = [(lat_ref, lat_held, lat_out)]
    for k in range(0, TILE, TILE // 4):
        part = pl.ds(k, TILE // 4)
        steps.append((sym_ref.at[part], sym_held.at[part], sym_out.at[part]))
    takes = [
        pltpu.make_async_copy(src, mid, sem_in.at[k]) for k, (src, mid, _) in enumerate(steps)
    ]
    gives = [
        pltpu.make_async_copy(mid, dst, sem_out.at[k]) for k, (_, mid, dst) in enumerate(steps)
    ]
    for take in takes:
        take.start()
    for take, give in zip(takes, gives):
        take.wait()
        give.start()
    for give in gives:
        give.wait()


def body(
    contact_map,
    embed_weight,
    embed_bias,
    conv_weight,
    conv_bias,
    mix_weight,
    mix_bias,
    proj_weight,
    proj_bias,
    up_weight,
    up_bias,
    down_weight,
    down_bias,
):
    n = lax.axis_size("col")
    rows_each = TILE // n
    latent_width, hidden_width = up_weight.shape
    vmem = pl.BlockSpec(memory_space=pltpu.VMEM)
    hbm = pl.BlockSpec(memory_space=pltpu.HBM)
    dma = pltpu.SemaphoreType.DMA
    args = (
        contact_map,
        embed_weight,
        embed_bias.reshape(1, CH),
        conv_weight.reshape(LAYERS, 9 * CH, CH),
        conv_bias,
        mix_weight,
        mix_bias.reshape(1, CH),
        proj_weight,
        proj_bias.reshape(1, latent_width),
        up_weight,
        up_bias.reshape(1, hidden_width),
        down_weight,
        down_bias.reshape(1, latent_width),
    )
    shapes = (
        jax.ShapeDtypeStruct((rows_each, latent_width), BF16),
        jax.ShapeDtypeStruct((TILE, TILE, CH), BF16),
    )
    done = pl.pallas_call(
        functools.partial(kernel, n),
        out_shape=shapes,
        in_specs=[hbm] * len(args),
        out_specs=(hbm, hbm),
        scratch_shapes=[pltpu.VMEM(a.shape, a.dtype) for a in args]
        + [
            pltpu.VMEM((TILE * PATCH, TILE * PATCH), F32),
            pltpu.VMEM((4, TILE, 128), BF16),
            pltpu.VMEM((4, TILE, 128), BF16),
            pltpu.VMEM((6, TILE + 2 * PAD, 128), BF16),
            pltpu.VMEM((6, TILE + 2 * PAD, 128), BF16),
            pltpu.VMEM((3, 2, 19, SUB, CH), BF16),
            pltpu.VMEM((3, 2, 18, SUB, CH), BF16),
            pltpu.VMEM((3, 2, 17, TILE, CH), BF16),
            pltpu.VMEM((TILE, TILE, CH), BF16),
            pltpu.VMEM((2, 9 * SUB, 2 * CH), F32),
            pltpu.VMEM(shapes[1].shape, BF16),
            pltpu.VMEM(shapes[0].shape, BF16),
            pltpu.VMEM((n, rows_each, CH), F32),
            pltpu.VMEM((n, rows_each, CH), F32),
            dma((9,)),
            dma((9,)),
            dma((9,)),
            dma((9,)),
            dma((n,)),
            dma((n,)),
            dma((len(args),)),
            dma((5,)),
        ],
        compiler_params=pltpu.CompilerParams(
            collective_id=0, has_side_effects=True, vmem_limit_bytes=67043328
        ),
    )(*args)
    return pl.pallas_call(
        hand_over,
        out_shape=shapes,
        in_specs=[hbm, hbm],
        out_specs=(hbm, hbm),
        scratch_shapes=[pltpu.VMEM(shape.shape, BF16) for shape in shapes]
        + [dma((5,)), dma((5,))],
    )(*done)


def solution(mesh):
    return jax.shard_map(
        body,
        mesh=mesh,
        in_specs=(P("row", "col"),) + (P(),) * 12,
        out_specs=(P(("row", "col"), None), P("row", "col", None)),
        check_vma=False,
    )
```

```python
import functools

import jax
import jax.numpy as jnp
from jax import lax
from jax.experimental import pallas as pl
from jax.experimental.pallas import tpu as pltpu
from jax.sharding import PartitionSpec as P

PATCH = 4
LAYERS = 3
TILE = 32
BLK = 8
PAD = 8
SUB = 48
CH = 128
MESH = pl.DeviceIdType.MESH
F32 = jnp.float32
BF16 = jnp.bfloat16
CUTS = [[(0, 6), (6, 6), (12, 6)], [(0, 6), (6, 6), (12, 5)], [(0, 6), (6, 5), (11, 5)]]
OFFSETS = [(dl, ds) for dl in (-1, 0, 1) for ds in (-1, 0, 1)]


def gelu_of_half(half):
    inner = half * (2 * 0.7978845608028654 + (8 * 0.7978845608028654 * 0.044715) * (half * half))
    return half + half * jnp.tanh(inner)


def gelu(x):
    return gelu_of_half(0.5 * x)


def lead_src(d):
    return {-1: pl.ds(3, 1), 0: pl.ds(0, 4), 1: pl.ds(0, 1)}[d]


def lead_dst(d):
    return {-1: pl.ds(0, 1), 0: pl.ds(1, 4), 1: pl.ds(5, 1)}[d]


def sub_src(d):
    return {-1: pl.ds(TILE - PAD, PAD), 0: pl.ds(0, TILE), 1: pl.ds(0, PAD)}[d]


def sub_dst(d):
    return {-1: pl.ds(0, PAD), 0: pl.ds(PAD, TILE), 1: pl.ds(PAD + TILE, PAD)}[d]


def kernel(
    n,
    x_hbm,
    ew_hbm,
    eb_hbm,
    cw_hbm,
    cb_hbm,
    mw_hbm,
    mb_hbm,
    pw_hbm,
    pb_hbm,
    uw_hbm,
    ub_hbm,
    dw_hbm,
    db_hbm,
    lat_hbm,
    sym_hbm,
    x_ref,
    ew_ref,
    eb_ref,
    cw,
    cb_ref,
    mw_ref,
    mb_ref,
    pw,
    pb_ref,
    uw,
    ub_ref,
    dw,
    db_ref,
    xt,
    own_p,
    own_q,
    near_h,
    far_h,
    f0,
    f1,
    f2,
    f3,
    acc,
    stage,
    symb,
    lat_ref,
    part,
    got,
    near_ss,
    near_rs,
    far_ss,
    far_rs,
    red_ss,
    red_rs,
    wsem,
    osem,
):
    r = lax.axis_index("row")
    c = lax.axis_index("col")
    rows_each = TILE // n

    held = [
        (x_hbm, x_ref),
        (ew_hbm, ew_ref),
        (eb_hbm, eb_ref),
        (cw_hbm, cw),
        (cb_hbm, cb_ref),
        (mw_hbm, mw_ref),
        (mb_hbm, mb_ref),
        (pw_hbm, pw),
        (pb_hbm, pb_ref),
        (uw_hbm, uw),
        (ub_hbm, ub_ref),
        (dw_hbm, dw),
        (db_hbm, db_ref),
    ]
    def inside(a, b):
        return (a >= 0) & (a < n) & (b >= 0) & (b < n)

    barrier = pltpu.get_barrier_semaphore()
    count = jnp.int32(n - 1)

    def greet(a, b):
        pl.semaphore_signal(barrier, inc=1, device_id=(a, b), device_id_type=MESH)

    for dl, ds in OFFSETS:
        far_ok = inside(c + ds, r + dl) & ((c + ds != r) | (r + dl != c))
        pl.when(far_ok)(functools.partial(greet, c + ds, r + dl))
        count += far_ok.astype(jnp.int32)
    for dl, ds in OFFSETS:
        if dl or ds:
            near_ok = inside(r + dl, c + ds)
            pl.when(near_ok)(functools.partial(greet, r + dl, c + ds))
            count += near_ok.astype(jnp.int32)
    for k in range(1, n):
        greet(r, lax.rem(c + k, n))

    loads = [pltpu.make_async_copy(src, dst, wsem.at[k]) for k, (src, dst) in enumerate(held)]
    for load in loads:
        load.start()
    loads[0].wait()
    xt[...] = x_ref[...].T
    y_p = jnp.concatenate([x_ref[pl.ds(s, TILE, stride=PATCH), :] for s in range(PATCH)], axis=1)
    y_q = jnp.concatenate([xt[pl.ds(s, TILE, stride=PATCH), :] for s in range(PATCH)], axis=1)
    y = jnp.concatenate([y_p, y_q], axis=0).astype(BF16)
    k = lax.broadcasted_iota(jnp.int32, (512, 512), 0)
    target = ((k >> 5) & 3) * 128 + ((k >> 2) & 7) * 16 + (k >> 7) * 4 + (k & 3)
    perm = (lax.broadcasted_iota(jnp.int32, (512, 512), 1) == target).astype(F32).astype(BF16)
    z = jnp.dot(y, perm, preferred_element_type=F32).astype(BF16)
    for h in range(4):
        p_h = z[:TILE, h * 128 : (h + 1) * 128]
        q_h = z[TILE:, h * 128 : (h + 1) * 128]
        own_p[h] = p_h
        own_q[h] = q_h
        near_h[h + 1, PAD : PAD + TILE, :] = q_h

    pr = lax.broadcasted_iota(jnp.int32, (128, 16), 0)
    pc = lax.broadcasted_iota(jnp.int32, (128, 16), 1)
    rid = lax.broadcasted_iota(jnp.int32, (128, 128), 0) >> 4

    def block_diagonal(swap):
        row = (pr & 3) * 4 + ((pr >> 2) & 3) if swap else pr & 15
        pick = (pc == row).astype(F32).astype(BF16)
        tiled = jnp.dot(pick, ew_ref[...], preferred_element_type=F32)
        return jnp.concatenate(
            [jnp.where(rid == b, tiled, 0.0).astype(BF16) for b in range(BLK)], axis=1
        )

    pl.semaphore_wait(barrier, count)

    def message(src, dst, ss, rs, dl, ds, a, b):
        i = (dl + 1) * 3 + ds + 1
        return pltpu.make_async_remote_copy(
            src_ref=src.at[lead_src(dl), sub_src(ds), :],
            dst_ref=dst.at[lead_dst(dl), sub_dst(ds), :],
            send_sem=ss.at[i],
            recv_sem=rs.at[i],
            device_id=(a, b),
            device_id_type=MESH,
        )

    far_out, far_in, near_out, near_in = [], [], [], []
    for dl, ds in OFFSETS:
        a, b = c - dl, r - ds
        ok = inside(a, b) & ((a != r) | (b != c))
        out = message(own_p, far_h, far_ss, far_rs, dl, ds, a, b)
        far_out.append((ok, out))
        pl.when(ok)(out.start)
        ok_in = inside(c + ds, r + dl) & ((c + ds != r) | (r + dl != c))
        far_in.append((ok_in, message(own_p, far_h, far_ss, far_rs, dl, ds, r, c)))
    for dl, ds in OFFSETS:
        if dl or ds:
            a, b = r - dl, c - ds
            ok = inside(a, b)
            out = message(own_q, near_h, near_ss, near_rs, dl, ds, a, b)
            near_out.append((ok, out))
            pl.when(ok)(out.start)
            near_in.append(
                (inside(r + dl, c + ds), message(own_q, near_h, near_ss, near_rs, dl, ds, r, c))
            )

    for load in loads[1:]:
        load.wait()
    for layer in range(LAYERS):
        for k in range(9):
            tap_rows = pl.ds(k * CH, CH)
            cw[layer, tap_rows, :] = cw[layer, tap_rows, :] * jnp.bfloat16(0.5)
    mw_ref[...] = mw_ref[...] * jnp.bfloat16(0.5)
    cb_half = cb_ref[...] * 0.5
    mb_half = mb_ref[...] * 0.5

    def keep(dl, ds):
        far_h[lead_dst(dl), sub_dst(ds), :] = own_p[lead_src(dl), sub_src(ds), :]

    pl.when(r == c)(functools.partial(keep, 0, 0))
    pl.when(c == r + 1)(functools.partial(keep, 1, -1))
    pl.when(c == r - 1)(functools.partial(keep, -1, 1))

    sub_cell = c * TILE - 8 + lax.broadcasted_iota(jnp.int32, (SUB, 1), 0)
    sub_ok = (sub_cell >= 0) & (sub_cell < n * TILE)

    keep_sub = jnp.broadcast_to(sub_ok.astype(F32), (SUB, CH))

    def lead_ok(first):
        lead = r * TILE + first
        return (lead >= 0) & (lead < n * TILE)

    def masked(value, first):
        keep = keep_sub
        if first < 0 or first >= TILE:
            keep = keep * lead_ok(first).astype(F32)
        return value * keep

    def put(ref, parity, at, value, cut=False):
        line = stage.at[parity, at]
        line[8 : 8 + SUB, :] = value
        first, rows = (16, TILE) if cut else (8, SUB)
        for s in range(3):
            ref[s, parity, at] = line[pl.ds(first + s - 1, rows), :].astype(BF16)

    def embed(patches, diag):
        for h in range(6):
            first, last = (5, 8) if h == 0 else (0, 3) if h == 5 else (0, 8)
            wide = jnp.dot(patches[h], diag, preferred_element_type=F32)
            for b in range(first, last):
                at = h * BLK + b - 5
                cells = wide[:, b * CH : (b + 1) * CH] + eb_ref[...]
                put(f0, at % 2, at // 2, jnp.where(sub_ok & lead_ok(at - 3), cells, 0.0))

    def conv(layer, src, at, pairs, lead_is_row, slot):
        def tap(lead, sub):
            if lead < 0 or lead > 2:
                return jnp.zeros((CH, CH), BF16)
            k = lead * 3 + sub if lead_is_row else sub * 3 + lead
            return cw[layer, k * CH : (k + 1) * CH, :]

        pieces, taps = [], []
        for lead in range(4):
            for sub in range(3):
                first = at + lead // 2
                piece = src[sub, lead % 2, first : first + pairs]
                pieces.append(piece.reshape(pairs * piece.shape[1], CH))
                taps.append(jnp.concatenate([tap(lead, sub), tap(lead - 1, sub)], axis=1))
        lhs = jnp.concatenate(pieces, axis=1)
        rows = pairs * SUB if layer < 2 else pairs * TILE
        acc[slot, :rows] = jnp.dot(lhs, jnp.concatenate(taps, axis=0), preferred_element_type=F32)

    def cell_row(layer, slot, k, h):
        each = SUB if layer < 2 else TILE
        total = acc[slot, k * each : (k + 1) * each, h * CH : (h + 1) * CH]
        return gelu_of_half(total + cb_half[layer : layer + 1])

    def features(lead_is_row, finish, finish_block):
        maps = [(f0, f1), (f1, f2), (f2, None)]
        tasks = [(layer, at, pairs) for layer in range(LAYERS) for at, pairs in CUTS[layer]]

        def multiply(t):
            layer, at, pairs = tasks[t]
            conv(layer, maps[layer][0], at, pairs, lead_is_row, t % 2)

        multiply(0)
        for t, (layer, at, pairs) in enumerate(tasks):
            if t + 1 < len(tasks):
                multiply(t + 1)
            for k in range(pairs):
                for h in (0, 1):
                    v = cell_row(layer, t % 2, k, h)
                    if layer == LAYERS - 1:
                        finish(at + k, h, v.astype(BF16))
                    else:
                        lead = 2 * (at + k) + h - 2 + layer
                        put(maps[layer][1], h, at + k, masked(v, lead), cut=layer == 1)
            if layer == LAYERS - 1:
                finish_block(2 * at, 2 * pairs)

    diag_q = block_diagonal(True)
    for ok, got_in in near_in:
        pl.when(ok)(got_in.wait_recv)
    embed(near_h, diag_q)

    def keep_own(m, h, value):
        f3[2 * m + h] = value

    features(True, keep_own, lambda first, count_l: None)

    diag_p = block_diagonal(False)
    for ok, got_in in far_in:
        pl.when(ok)(got_in.wait_recv)
    embed(far_h, diag_p)

    outs = []

    def finish_far(m, h, value):
        i = 2 * m + h
        symb[i] = ((f3[i].astype(F32) + value.astype(F32)) * 0.5).astype(BF16)

    def mix_block(first, count_l):
        rows = pl.ds(first, count_l)
        out = pltpu.make_async_copy(symb.at[rows], sym_hbm.at[rows], osem.at[len(outs)])
        out.start()
        outs.append(out)
        mixed = jnp.dot(
            symb[rows].reshape(count_l * TILE, CH), mw_ref[...], preferred_element_type=F32
        )
        sums = jnp.sum(gelu_of_half(mixed + mb_half).reshape(count_l, TILE, CH), axis=1)
        for k in range(count_l):
            row = first + k
            part[row // rows_each, row % rows_each : row % rows_each + 1] = sums[k : k + 1]

    features(False, finish_far, mix_block)

    moves = []
    for k in range(1, n):
        to = lax.rem(c + k, n)
        move = pltpu.make_async_remote_copy(
            src_ref=part.at[to],
            dst_ref=got.at[k],
            send_sem=red_ss.at[k],
            recv_sem=red_rs.at[k],
            device_id=(r, to),
            device_id_type=MESH,
        )
        move.start()
        moves.append(move)
    for move in moves:
        move.wait_recv()
    summed = part[c]
    for k in range(1, n):
        summed = summed + got[k]
    pooled = (summed / (n * TILE)).astype(BF16)
    latent = jnp.dot(pooled, pw[...], preferred_element_type=F32) + pb_ref[...]
    hidden = gelu(jnp.dot(latent.astype(BF16), uw[...], preferred_element_type=F32) + ub_ref[...])
    result = latent + jnp.dot(hidden.astype(BF16), dw[...], preferred_element_type=F32) + db_ref[...]
    lat_ref[...] = result.astype(BF16)
    out = pltpu.make_async_copy(lat_ref, lat_hbm, osem.at[len(outs)])
    out.start()
    outs.append(out)

    for move in moves:
        move.wait_send()
    for ok, out in far_out + near_out:
        pl.when(ok)(out.wait_send)
    for out in outs:
        out.wait()


def hand_over(lat_ref, sym_ref, lat_out, sym_out, lat_held, sym_held, sem_in, sem_out):
    steps = [(lat_ref, lat_held, lat_out)]
    for k in range(0, TILE, TILE // 4):
        part = pl.ds(k, TILE // 4)
        steps.append((sym_ref.at[part], sym_held.at[part], sym_out.at[part]))
    takes = [
        pltpu.make_async_copy(src, mid, sem_in.at[k]) for k, (src, mid, _) in enumerate(steps)
    ]
    gives = [
        pltpu.make_async_copy(mid, dst, sem_out.at[k]) for k, (_, mid, dst) in enumerate(steps)
    ]
    for take in takes:
        take.start()
    for take, give in zip(takes, gives):
        take.wait()
        give.start()
    for give in gives:
        give.wait()


def body(
    contact_map,
    embed_weight,
    embed_bias,
    conv_weight,
    conv_bias,
    mix_weight,
    mix_bias,
    proj_weight,
    proj_bias,
    up_weight,
    up_bias,
    down_weight,
    down_bias,
):
    n = lax.axis_size("col")
    rows_each = TILE // n
    latent_width, hidden_width = up_weight.shape
    vmem = pl.BlockSpec(memory_space=pltpu.VMEM)
    hbm = pl.BlockSpec(memory_space=pltpu.HBM)
    dma = pltpu.SemaphoreType.DMA
    args = (
        contact_map,
        embed_weight,
        embed_bias.reshape(1, CH),
        conv_weight.reshape(LAYERS, 9 * CH, CH),
        conv_bias,
        mix_weight,
        mix_bias.reshape(1, CH),
        proj_weight,
        proj_bias.reshape(1, latent_width),
        up_weight,
        up_bias.reshape(1, hidden_width),
        down_weight,
        down_bias.reshape(1, latent_width),
    )
    shapes = (
        jax.ShapeDtypeStruct((rows_each, latent_width), BF16),
        jax.ShapeDtypeStruct((TILE, TILE, CH), BF16),
    )
    done = pl.pallas_call(
        functools.partial(kernel, n),
        out_shape=shapes,
        in_specs=[hbm] * len(args),
        out_specs=(hbm, hbm),
        scratch_shapes=[pltpu.VMEM(a.shape, a.dtype) for a in args]
        + [
            pltpu.VMEM((TILE * PATCH, TILE * PATCH), F32),
            pltpu.VMEM((4, TILE, 128), BF16),
            pltpu.VMEM((4, TILE, 128), BF16),
            pltpu.VMEM((6, TILE + 2 * PAD, 128), BF16),
            pltpu.VMEM((6, TILE + 2 * PAD, 128), BF16),
            pltpu.VMEM((3, 2, 19, SUB, CH), BF16),
            pltpu.VMEM((3, 2, 18, SUB, CH), BF16),
            pltpu.VMEM((3, 2, 17, TILE, CH), BF16),
            pltpu.VMEM((TILE, TILE, CH), BF16),
            pltpu.VMEM((2, 6 * SUB, 2 * CH), F32),
            pltpu.VMEM((2, 19, SUB + 16, CH), F32),
            pltpu.VMEM(shapes[1].shape, BF16),
            pltpu.VMEM(shapes[0].shape, BF16),
            pltpu.VMEM((n, rows_each, CH), F32),
            pltpu.VMEM((n, rows_each, CH), F32),
            dma((9,)),
            dma((9,)),
            dma((9,)),
            dma((9,)),
            dma((n,)),
            dma((n,)),
            dma((len(args),)),
            dma((5,)),
        ],
        compiler_params=pltpu.CompilerParams(
            collective_id=0, has_side_effects=True, vmem_limit_bytes=67043328
        ),
    )(*args)
    return pl.pallas_call(
        hand_over,
        out_shape=shapes,
        in_specs=[hbm, hbm],
        out_specs=(hbm, hbm),
        scratch_shapes=[pltpu.VMEM(shape.shape, BF16) for shape in shapes]
        + [dma((5,)), dma((5,))],
    )(*done)


def solution(mesh):
    return jax.shard_map(
        body,
        mesh=mesh,
        in_specs=(P("row", "col"),) + (P(),) * 12,
        out_specs=(P(("row", "col"), None), P("row", "col", None)),
        check_vma=False,
    )
```

```python
import functools

import jax
import jax.numpy as jnp
from jax import lax
from jax.experimental import pallas as pl
from jax.experimental.pallas import tpu as pltpu
from jax.sharding import PartitionSpec as P

PATCH = 4
LAYERS = 3
TILE = 32
BLK = 8
PAD = 8
SUB = 48
CH = 128
MESH = pl.DeviceIdType.MESH
F32 = jnp.float32
BF16 = jnp.bfloat16
CUTS = [[(0, 6), (6, 6), (12, 6)], [(0, 6), (6, 6), (12, 5)], [(0, 6), (6, 5), (11, 5)]]
OFFSETS = [(dl, ds) for dl in (-1, 0, 1) for ds in (-1, 0, 1)]


def gelu_of_half(half):
    inner = half * (2 * 0.7978845608028654 + (8 * 0.7978845608028654 * 0.044715) * (half * half))
    return half + half * jnp.tanh(inner)


def gelu(x):
    return gelu_of_half(0.5 * x)


def lead_src(d):
    return {-1: pl.ds(3, 1), 0: pl.ds(0, 4), 1: pl.ds(0, 1)}[d]


def lead_dst(d):
    return {-1: pl.ds(0, 1), 0: pl.ds(1, 4), 1: pl.ds(5, 1)}[d]


def sub_src(d):
    return {-1: pl.ds(TILE - PAD, PAD), 0: pl.ds(0, TILE), 1: pl.ds(0, PAD)}[d]


def sub_dst(d):
    return {-1: pl.ds(0, PAD), 0: pl.ds(PAD, TILE), 1: pl.ds(PAD + TILE, PAD)}[d]


def kernel(
    n,
    x_hbm,
    ew_hbm,
    eb_hbm,
    cw_hbm,
    cb_hbm,
    mw_hbm,
    mb_hbm,
    pw_hbm,
    pb_hbm,
    uw_hbm,
    ub_hbm,
    dw_hbm,
    db_hbm,
    lat_hbm,
    sym_hbm,
    x_ref,
    ew_ref,
    eb_ref,
    cw,
    cb_ref,
    mw_ref,
    mb_ref,
    pw,
    pb_ref,
    uw,
    ub_ref,
    dw,
    db_ref,
    xt,
    own_p,
    own_q,
    near_h,
    far_h,
    side_p,
    side_q,
    near_side,
    far_side,
    pack,
    line_buf,
    f0,
    f1,
    f2,
    f3,
    acc,
    stage,
    symb,
    lat_ref,
    part,
    got,
    near_ss,
    near_rs,
    far_ss,
    far_rs,
    red_ss,
    red_rs,
    wsem,
    osem,
):
    r = lax.axis_index("row")
    c = lax.axis_index("col")
    rows_each = TILE // n

    held = [
        (x_hbm, x_ref),
        (ew_hbm, ew_ref),
        (eb_hbm, eb_ref),
        (cw_hbm, cw),
        (cb_hbm, cb_ref),
        (mw_hbm, mw_ref),
        (mb_hbm, mb_ref),
        (pw_hbm, pw),
        (pb_hbm, pb_ref),
        (uw_hbm, uw),
        (ub_hbm, ub_ref),
        (dw_hbm, dw),
        (db_hbm, db_ref),
    ]
    def inside(a, b):
        return (a >= 0) & (a < n) & (b >= 0) & (b < n)

    barrier = pltpu.get_barrier_semaphore()
    count = jnp.int32(n - 1)

    def greet(a, b):
        pl.semaphore_signal(barrier, inc=1, device_id=(a, b), device_id_type=MESH)

    for dl, ds in OFFSETS:
        far_ok = inside(c + ds, r + dl) & ((c + ds != r) | (r + dl != c))
        pl.when(far_ok)(functools.partial(greet, c + ds, r + dl))
        count += far_ok.astype(jnp.int32)
    for dl, ds in OFFSETS:
        if dl or ds:
            near_ok = inside(r + dl, c + ds)
            pl.when(near_ok)(functools.partial(greet, r + dl, c + ds))
            count += near_ok.astype(jnp.int32)
    for k in range(1, n):
        greet(r, lax.rem(c + k, n))

    loads = [pltpu.make_async_copy(src, dst, wsem.at[k]) for k, (src, dst) in enumerate(held)]
    for load in loads:
        load.start()
    loads[0].wait()
    xt[...] = x_ref[...].T
    y_p = jnp.concatenate([x_ref[pl.ds(s, TILE, stride=PATCH), :] for s in range(PATCH)], axis=1)
    y_q = jnp.concatenate([xt[pl.ds(s, TILE, stride=PATCH), :] for s in range(PATCH)], axis=1)
    y = jnp.concatenate([y_p, y_q], axis=0).astype(BF16)
    k = lax.broadcasted_iota(jnp.int32, (512, 512), 0)
    target = ((k >> 5) & 3) * 128 + ((k >> 2) & 7) * 16 + (k >> 7) * 4 + (k & 3)
    perm = (lax.broadcasted_iota(jnp.int32, (512, 512), 1) == target).astype(F32).astype(BF16)
    z = jnp.dot(y, perm, preferred_element_type=F32)
    left = lax.broadcasted_iota(jnp.int32, (16, 128), 1) < 64
    for m, (own, side) in enumerate([(own_p, side_p), (own_q, side_q)]):
        slabs = [z[m * TILE : (m + 1) * TILE, h * 128 : (h + 1) * 128] for h in range(4)]
        for h in range(4):
            own[h] = slabs[h].astype(BF16)
            if m == 1:
                near_h[h + 1, PAD : PAD + TILE, :] = slabs[h].astype(BF16)
            pack[2 * m, 4 * h : 4 * h + 4, :] = slabs[h][TILE - 4 :, :]
            pack[2 * m + 1, 4 * h : 4 * h + 4, :] = slabs[h][:4, :]
        side[0] = pack[2 * m].astype(BF16)
        side[1] = pack[2 * m + 1].astype(BF16)
        end, start = slabs[3], slabs[0]
        side[2] = jnp.where(left, pltpu.roll(end[:16], 64, 1), end[16:]).astype(BF16)
        side[3] = jnp.where(left, start[:16], pltpu.roll(start[16:], 64, 1)).astype(BF16)

    pr = lax.broadcasted_iota(jnp.int32, (128, 16), 0)
    pc = lax.broadcasted_iota(jnp.int32, (128, 16), 1)
    rid = lax.broadcasted_iota(jnp.int32, (128, 128), 0) >> 4

    def block_diagonal(swap):
        row = (pr & 3) * 4 + ((pr >> 2) & 3) if swap else pr & 15
        pick = (pc == row).astype(F32).astype(BF16)
        tiled = jnp.dot(pick, ew_ref[...], preferred_element_type=F32)
        return jnp.concatenate(
            [jnp.where(rid == b, tiled, 0.0).astype(BF16) for b in range(BLK)], axis=1
        )

    pl.semaphore_wait(barrier, count)

    def message(src, dst, ss, rs, dl, ds, a, b):
        i = (dl + 1) * 3 + ds + 1
        if (dl == 0) != (ds == 0):
            k = (ds + 1) // 2 if dl == 0 else 2 + (dl + 1) // 2
            src_part, dst_part = src[1].at[k], dst[1].at[k]
        else:
            src_part = src[0].at[lead_src(dl), sub_src(ds), :]
            dst_part = dst[0].at[lead_dst(dl), sub_dst(ds), :]
        return pltpu.make_async_remote_copy(
            src_ref=src_part,
            dst_ref=dst_part,
            send_sem=ss.at[i],
            recv_sem=rs.at[i],
            device_id=(a, b),
            device_id_type=MESH,
        )

    far_out, far_in, near_out, near_in = [], [], [], []
    for dl, ds in OFFSETS:
        a, b = c - dl, r - ds
        ok = inside(a, b) & ((a != r) | (b != c))
        out = message((own_p, side_p), (far_h, far_side), far_ss, far_rs, dl, ds, a, b)
        far_out.append((ok, out))
        pl.when(ok)(out.start)
        ok_in = inside(c + ds, r + dl) & ((c + ds != r) | (r + dl != c))
        far_in.append((ok_in, message((own_p, side_p), (far_h, far_side), far_ss, far_rs, dl, ds, r, c)))
    for dl, ds in OFFSETS:
        if dl or ds:
            a, b = r - dl, c - ds
            ok = inside(a, b)
            out = message((own_q, side_q), (near_h, near_side), near_ss, near_rs, dl, ds, a, b)
            near_out.append((ok, out))
            pl.when(ok)(out.start)
            near_in.append(
                (inside(r + dl, c + ds), message((own_q, side_q), (near_h, near_side), near_ss, near_rs, dl, ds, r, c))
            )

    for load in loads[1:]:
        load.wait()
    for layer in range(LAYERS):
        for k in range(9):
            tap_rows = pl.ds(k * CH, CH)
            cw[layer, tap_rows, :] = cw[layer, tap_rows, :] * jnp.bfloat16(0.5)
    mw_ref[...] = mw_ref[...] * jnp.bfloat16(0.5)
    cb_half = cb_ref[...] * 0.5
    mb_half = mb_ref[...] * 0.5

    def keep(dl, ds):
        far_h[lead_dst(dl), sub_dst(ds), :] = own_p[lead_src(dl), sub_src(ds), :]

    pl.when(r == c)(functools.partial(keep, 0, 0))
    pl.when(c == r + 1)(functools.partial(keep, 1, -1))
    pl.when(c == r - 1)(functools.partial(keep, -1, 1))

    sub_cell = c * TILE - 8 + lax.broadcasted_iota(jnp.int32, (SUB, 1), 0)
    sub_ok = (sub_cell >= 0) & (sub_cell < n * TILE)

    keep_sub = jnp.broadcast_to(sub_ok.astype(F32), (SUB, CH))

    def lead_ok(first):
        lead = r * TILE + first
        return (lead >= 0) & (lead < n * TILE)

    def masked(value, first):
        keep = keep_sub
        if first < 0 or first >= TILE:
            keep = keep * lead_ok(first).astype(F32)
        return value * keep

    def put(ref, parity, at, value, cut=False):
        line = stage.at[parity, at]
        line[8 : 8 + SUB, :] = value
        first, rows = (16, TILE) if cut else (8, SUB)
        for s in range(3):
            ref[s, parity, at] = line[pl.ds(first + s - 1, rows), :].astype(BF16)

    def embed(patches, sides, diag):
        up, down = sides[0].astype(F32), sides[1].astype(F32)
        for h in range(6):
            first, last = (5, 8) if h == 0 else (0, 3) if h == 5 else (0, 8)
            line = line_buf.at[h]
            if 0 < h < 5:
                line[PAD - 4 : PAD, :] = up[4 * h - 4 : 4 * h]
                line[PAD : PAD + TILE, :] = patches[h, PAD : PAD + TILE, :].astype(F32)
                line[PAD + TILE : PAD + TILE + 4, :] = down[4 * h - 4 : 4 * h]
            else:
                half = sides[2 if h == 0 else 3].astype(F32)
                turned = pltpu.roll(half, 64, 1)
                line[:PAD, :] = patches[h, :PAD, :].astype(F32)
                line[PAD : PAD + 16, :] = turned if h == 0 else half
                line[PAD + 16 : PAD + 32, :] = half if h == 0 else turned
                line[PAD + TILE :, :] = patches[h, PAD + TILE :, :].astype(F32)
            wide = jnp.dot(line[...].astype(BF16), diag, preferred_element_type=F32)
            for b in range(first, last):
                at = h * BLK + b - 5
                cells = wide[:, b * CH : (b + 1) * CH] + eb_ref[...]
                put(f0, at % 2, at // 2, jnp.where(sub_ok & lead_ok(at - 3), cells, 0.0))

    def conv(layer, src, at, pairs, lead_is_row, slot):
        def tap(lead, sub):
            if lead < 0 or lead > 2:
                return jnp.zeros((CH, CH), BF16)
            k = lead * 3 + sub if lead_is_row else sub * 3 + lead
            return cw[layer, k * CH : (k + 1) * CH, :]

        pieces, taps = [], []
        for lead in range(4):
            for sub in range(3):
                first = at + lead // 2
                piece = src[sub, lead % 2, first : first + pairs]
                pieces.append(piece.reshape(pairs * piece.shape[1], CH))
                taps.append(jnp.concatenate([tap(lead, sub), tap(lead - 1, sub)], axis=1))
        lhs = jnp.concatenate(pieces, axis=1)
        rows = pairs * SUB if layer < 2 else pairs * TILE
        acc[slot, :rows] = jnp.dot(lhs, jnp.concatenate(taps, axis=0), preferred_element_type=F32)

    def cell_row(layer, slot, k, h):
        each = SUB if layer < 2 else TILE
        total = acc[slot, k * each : (k + 1) * each, h * CH : (h + 1) * CH]
        return gelu_of_half(total + cb_half[layer : layer + 1])

    def features(lead_is_row, finish, finish_block):
        maps = [(f0, f1), (f1, f2), (f2, None)]
        tasks = [(layer, at, pairs) for layer in range(LAYERS) for at, pairs in CUTS[layer]]

        def multiply(t):
            layer, at, pairs = tasks[t]
            conv(layer, maps[layer][0], at, pairs, lead_is_row, t % 2)

        multiply(0)
        for t, (layer, at, pairs) in enumerate(tasks):
            if t + 1 < len(tasks):
                multiply(t + 1)
            for k in range(pairs):
                for h in (0, 1):
                    v = cell_row(layer, t % 2, k, h)
                    if layer == LAYERS - 1:
                        finish(at + k, h, v.astype(BF16))
                    else:
                        lead = 2 * (at + k) + h - 2 + layer
                        put(maps[layer][1], h, at + k, masked(v, lead), cut=layer == 1)
            if layer == LAYERS - 1:
                finish_block(2 * at, 2 * pairs)

    diag_q = block_diagonal(True)
    for ok, got_in in near_in:
        pl.when(ok)(got_in.wait_recv)
    embed(near_h, near_side, diag_q)

    def keep_own(m, h, value):
        f3[2 * m + h] = value

    features(True, keep_own, lambda first, count_l: None)

    diag_p = block_diagonal(False)
    for ok, got_in in far_in:
        pl.when(ok)(got_in.wait_recv)
    embed(far_h, far_side, diag_p)

    outs = []

    def finish_far(m, h, value):
        i = 2 * m + h
        symb[i] = ((f3[i].astype(F32) + value.astype(F32)) * 0.5).astype(BF16)

    def mix_block(first, count_l):
        rows = pl.ds(first, count_l)
        out = pltpu.make_async_copy(symb.at[rows], sym_hbm.at[rows], osem.at[len(outs)])
        out.start()
        outs.append(out)
        mixed = jnp.dot(
            symb[rows].reshape(count_l * TILE, CH), mw_ref[...], preferred_element_type=F32
        )
        sums = jnp.sum(gelu_of_half(mixed + mb_half).reshape(count_l, TILE, CH), axis=1)
        for k in range(count_l):
            row = first + k
            part[row // rows_each, row % rows_each : row % rows_each + 1] = sums[k : k + 1]

    features(False, finish_far, mix_block)

    moves = []
    for k in range(1, n):
        to = lax.rem(c + k, n)
        move = pltpu.make_async_remote_copy(
            src_ref=part.at[to],
            dst_ref=got.at[k],
            send_sem=red_ss.at[k],
            recv_sem=red_rs.at[k],
            device_id=(r, to),
            device_id_type=MESH,
        )
        move.start()
        moves.append(move)
    for move in moves:
        move.wait_recv()
    summed = part[c]
    for k in range(1, n):
        summed = summed + got[k]
    pooled = (summed / (n * TILE)).astype(BF16)
    latent = jnp.dot(pooled, pw[...], preferred_element_type=F32) + pb_ref[...]
    hidden = gelu(jnp.dot(latent.astype(BF16), uw[...], preferred_element_type=F32) + ub_ref[...])
    result = latent + jnp.dot(hidden.astype(BF16), dw[...], preferred_element_type=F32) + db_ref[...]
    lat_ref[...] = result.astype(BF16)
    out = pltpu.make_async_copy(lat_ref, lat_hbm, osem.at[len(outs)])
    out.start()
    outs.append(out)

    for move in moves:
        move.wait_send()
    for ok, out in far_out + near_out:
        pl.when(ok)(out.wait_send)
    for out in outs:
        out.wait()


def hand_over(lat_ref, sym_ref, lat_out, sym_out, lat_held, sym_held, sem_in, sem_out):
    steps = [(lat_ref, lat_held, lat_out)]
    for k in range(0, TILE, TILE // 4):
        part = pl.ds(k, TILE // 4)
        steps.append((sym_ref.at[part], sym_held.at[part], sym_out.at[part]))
    takes = [
        pltpu.make_async_copy(src, mid, sem_in.at[k]) for k, (src, mid, _) in enumerate(steps)
    ]
    gives = [
        pltpu.make_async_copy(mid, dst, sem_out.at[k]) for k, (_, mid, dst) in enumerate(steps)
    ]
    for take in takes:
        take.start()
    for take, give in zip(takes, gives):
        take.wait()
        give.start()
    for give in gives:
        give.wait()


def body(
    contact_map,
    embed_weight,
    embed_bias,
    conv_weight,
    conv_bias,
    mix_weight,
    mix_bias,
    proj_weight,
    proj_bias,
    up_weight,
    up_bias,
    down_weight,
    down_bias,
):
    n = lax.axis_size("col")
    rows_each = TILE // n
    latent_width, hidden_width = up_weight.shape
    vmem = pl.BlockSpec(memory_space=pltpu.VMEM)
    hbm = pl.BlockSpec(memory_space=pltpu.HBM)
    dma = pltpu.SemaphoreType.DMA
    args = (
        contact_map,
        embed_weight,
        embed_bias.reshape(1, CH),
        conv_weight.reshape(LAYERS, 9 * CH, CH),
        conv_bias,
        mix_weight,
        mix_bias.reshape(1, CH),
        proj_weight,
        proj_bias.reshape(1, latent_width),
        up_weight,
        up_bias.reshape(1, hidden_width),
        down_weight,
        down_bias.reshape(1, latent_width),
    )
    shapes = (
        jax.ShapeDtypeStruct((rows_each, latent_width), BF16),
        jax.ShapeDtypeStruct((TILE, TILE, CH), BF16),
    )
    done = pl.pallas_call(
        functools.partial(kernel, n),
        out_shape=shapes,
        in_specs=[hbm] * len(args),
        out_specs=(hbm, hbm),
        scratch_shapes=[pltpu.VMEM(a.shape, a.dtype) for a in args]
        + [
            pltpu.VMEM((TILE * PATCH, TILE * PATCH), F32),
            pltpu.VMEM((4, TILE, 128), BF16),
            pltpu.VMEM((4, TILE, 128), BF16),
            pltpu.VMEM((6, TILE + 2 * PAD, 128), BF16),
            pltpu.VMEM((6, TILE + 2 * PAD, 128), BF16),
            pltpu.VMEM((4, 16, 128), BF16),
            pltpu.VMEM((4, 16, 128), BF16),
            pltpu.VMEM((4, 16, 128), BF16),
            pltpu.VMEM((4, 16, 128), BF16),
            pltpu.VMEM((4, 16, 128), F32),
            pltpu.VMEM((6, TILE + 2 * PAD, 128), F32),
            pltpu.VMEM((3, 2, 19, SUB, CH), BF16),
            pltpu.VMEM((3, 2, 18, SUB, CH), BF16),
            pltpu.VMEM((3, 2, 17, TILE, CH), BF16),
            pltpu.VMEM((TILE, TILE, CH), BF16),
            pltpu.VMEM((2, 6 * SUB, 2 * CH), F32),
            pltpu.VMEM((2, 19, SUB + 16, CH), F32),
            pltpu.VMEM(shapes[1].shape, BF16),
            pltpu.VMEM(shapes[0].shape, BF16),
            pltpu.VMEM((n, rows_each, CH), F32),
            pltpu.VMEM((n, rows_each, CH), F32),
            dma((9,)),
            dma((9,)),
            dma((9,)),
            dma((9,)),
            dma((n,)),
            dma((n,)),
            dma((len(args),)),
            dma((5,)),
        ],
        compiler_params=pltpu.CompilerParams(
            collective_id=0, has_side_effects=True, vmem_limit_bytes=67043328
        ),
    )(*args)
    return pl.pallas_call(
        hand_over,
        out_shape=shapes,
        in_specs=[hbm, hbm],
        out_specs=(hbm, hbm),
        scratch_shapes=[pltpu.VMEM(shape.shape, BF16) for shape in shapes]
        + [dma((5,)), dma((5,))],
    )(*done)


def solution(mesh):
    return jax.shard_map(
        body,
        mesh=mesh,
        in_specs=(P("row", "col"),) + (P(),) * 12,
        out_specs=(P(("row", "col"), None), P("row", "col", None)),
        check_vma=False,
    )
```
